8 devices in a mesh: dp: 1 (over z), ep: 8 (over y, x, core).
Axes of the slice: x: 2, y: 2, z: 1, core: 2. Of those that a mesh axis runs over, the one named last changes fastest.
Arguments:
- tokens: bfloat16 [8, 512, 2048], P(('dp', 'ep'))
- w_query: bfloat16 [2048, 16, 256], P('ep')
- w_key: bfloat16 [2048, 16, 256], P('ep')
- w_value: bfloat16 [2048, 16, 256], P('ep')
- w_out: bfloat16 [4096, 2048], P('ep')
- w_router: float32 [2048, 512], replicated
- w_one: bfloat16 [512, 2048, 128], P('ep')
- w_three: bfloat16 [512, 2048, 128], P('ep')
- w_two: bfloat16 [512, 128, 2048], P('ep')
- expert_ids: int32 [8, 512, 10], P(('dp', 'ep'))
Outputs:
- output: bfloat16 [8, 512, 2048], P(('dp', 'ep'))
All inputs are finite; a program needn't handle non-finite values.
Results may differ from the reference program's by a relative error of at most 0.00951267.
Values are sent between devices in bfloat16 or wider.
A program may use at most 1 GiB of HBM per device.

```python
import jax
import jax.numpy as jnp
import numpy as np
from jax import lax

D = 2048
HEADS = 16
HEAD = 256
EXPERTS = 512
TOP = 10
FF = 128
TOK_DEV = 512
SEQ = 512
GROUP = 8

TOKENS = TOK_DEV * GROUP
N_SEQ = TOKENS // SEQ
CAP = 2 * TOK_DEV * TOP // EXPERTS
WIDTH = HEADS * HEAD
EPS = 1e-6


def draw_routing(route_key):
    mean_load = TOK_DEV * TOP // EXPERTS
    ranks = np.arange(EXPERTS)
    loads = np.where(ranks < EXPERTS // 4, 2 * mean_load, np.where(ranks < EXPERTS // 2, mean_load, mean_load // 2))
    rank_of_pos = np.repeat(ranks, loads)
    order_key, device_key = jax.random.split(route_key)
    expert_order = jax.random.permutation(order_key, EXPERTS)
    grid = expert_order[rank_of_pos].reshape(TOP, TOK_DEV).T

    def one_device(dev_key):
        perm_key, shift_key = jax.random.split(dev_key)
        token_order = jax.random.permutation(perm_key, TOK_DEV)
        shift = jax.random.randint(shift_key, (TOK_DEV, 1), 0, TOP)
        columns = (jnp.arange(TOP)[None, :] + shift) % TOP
        return jnp.take_along_axis(grid[token_order], columns, axis=1)

    routes = jax.vmap(one_device)(jax.random.split(device_key, GROUP))
    return routes.reshape(N_SEQ, SEQ, TOP).astype(jnp.int32)


def setup_inputs(seed: int = 0, part: int = 0) -> dict:
    root_key = jax.random.key(seed)
    part_keys = jax.random.split(jax.random.fold_in(root_key, part), 3)
    weight_keys = jax.random.split(root_key, 8)

    def gaussian(index, shape, scale):
        return scale * jax.random.normal(weight_keys[index], shape, jnp.float32)

    seq_base = jax.random.normal(part_keys[0], (N_SEQ, 1, D), jnp.float32)
    noise = jax.random.normal(part_keys[1], (N_SEQ, SEQ, D), jnp.float32)
    return {
        'tokens': (0.6 * seq_base + 0.8 * noise).astype(jnp.bfloat16),
        'w_query': gaussian(0, (D, HEADS, HEAD), 1.5 * D ** -0.5).astype(jnp.bfloat16),
        'w_key': gaussian(1, (D, HEADS, HEAD), 1.5 * D ** -0.5).astype(jnp.bfloat16),
        'w_value': gaussian(2, (D, HEADS, HEAD), D ** -0.5).astype(jnp.bfloat16),
        'w_out': gaussian(3, (WIDTH, D), WIDTH ** -0.5).astype(jnp.bfloat16),
        'w_router': gaussian(4, (D, EXPERTS), D ** -0.5),
        'w_one': gaussian(5, (EXPERTS, D, FF), D ** -0.5).astype(jnp.bfloat16),
        'w_three': gaussian(6, (EXPERTS, D, FF), D ** -0.5).astype(jnp.bfloat16),
        'w_two': gaussian(7, (EXPERTS, FF, D), 2.0 * FF ** -0.5).astype(jnp.bfloat16),
        'expert_ids': draw_routing(part_keys[2]),
    }


def rms_norm(vals):
    wide = vals.astype(jnp.float32)
    return wide * lax.rsqrt(jnp.mean(wide * wide, axis=-1, keepdims=True) + EPS)


def reference(tokens, w_query, w_key, w_value, w_out, w_router, w_one, w_three, w_two, expert_ids):
    flat_query = w_query.reshape(D, WIDTH)
    flat_key = w_key.reshape(D, WIDTH)
    flat_value = w_value.reshape(D, WIDTH)
    causal = jnp.arange(SEQ)[:, None] >= jnp.arange(SEQ)[None, :]

    def one_sequence(seq_tokens):
        normed = rms_norm(seq_tokens).astype(jnp.bfloat16)
        query = jnp.dot(normed, flat_query, preferred_element_type=jnp.float32).astype(jnp.bfloat16)
        keys = jnp.dot(normed, flat_key, preferred_element_type=jnp.float32).astype(jnp.bfloat16)
        values = jnp.dot(normed, flat_value, preferred_element_type=jnp.float32).astype(jnp.bfloat16)
        query = query.astype(jnp.float32).reshape(SEQ, HEADS, HEAD)
        keys = keys.astype(jnp.float32).reshape(SEQ, HEADS, HEAD)
        values = values.astype(jnp.float32).reshape(SEQ, HEADS, HEAD)
        scores = jnp.einsum('qhk,shk->hqs', query, keys) * HEAD ** -0.5
        scores = jnp.where(causal, scores, -jnp.inf)
        attn_weights = jax.nn.softmax(scores, axis=-1).astype(jnp.bfloat16).astype(jnp.float32)
        context = jnp.einsum('hqs,shk->qhk', attn_weights, values).astype(jnp.bfloat16)
        attn_out = jnp.dot(context.reshape(SEQ, WIDTH), w_out, preferred_element_type=jnp.float32)
        return (seq_tokens.astype(jnp.float32) + attn_out).astype(jnp.bfloat16)

    hidden = lax.map(one_sequence, tokens).reshape(TOKENS, D)
    normed = rms_norm(hidden)
    logits = jnp.dot(normed, w_router, preferred_element_type=jnp.float32)
    ids_flat = expert_ids.reshape(TOKENS, TOP)
    gates = jax.nn.softmax(jnp.take_along_axis(logits, ids_flat, axis=1), axis=-1)
    padded = jnp.concatenate([normed.astype(jnp.bfloat16), jnp.zeros((1, D), jnp.bfloat16)], axis=0)
    limit = GROUP * CAP

    def one_expert(total_mix, expert_pack):
        expert, first_w, third_w, second_w = expert_pack
        match = ids_flat == expert
        weight = jnp.sum(jnp.where(match, gates, 0.0), axis=1)
        rows = jnp.nonzero(jnp.any(match, axis=1), size=limit, fill_value=TOKENS)[0]
        picked = padded[rows]
        first = jnp.dot(picked, first_w, preferred_element_type=jnp.float32)
        third = jnp.dot(picked, third_w, preferred_element_type=jnp.float32)
        activated = (jax.nn.silu(first) * third).astype(jnp.bfloat16)
        result = jnp.dot(activated, second_w, preferred_element_type=jnp.float32).astype(jnp.bfloat16)
        scale = jnp.concatenate([weight, jnp.zeros((1,), jnp.float32)])[rows]
        total_mix = total_mix.at[rows].add(scale[:, None] * result.astype(jnp.float32), mode='drop')
        return total_mix, None

    total_mix, _ = lax.scan(one_expert, jnp.zeros((TOKENS, D), jnp.float32), (jnp.arange(EXPERTS), w_one, w_three, w_two))
    layer_out = (hidden.astype(jnp.float32) + total_mix).astype(jnp.bfloat16)
    return layer_out.reshape(N_SEQ, SEQ, D)
```

```python
import functools

import jax
import jax.numpy as jnp
from jax import lax
from jax.experimental import pallas as pl
from jax.experimental.pallas import tpu as pltpu
from jax.sharding import PartitionSpec as P

EPS = 1e-6
CAP = 20
LANES = 128
BATCH = 8


def rms_norm(vals):
    wide = vals.astype(jnp.float32)
    return wide * lax.rsqrt(jnp.mean(wide * wide, axis=-1, keepdims=True) + EPS)


def attention_layer(tokens, w_query, w_key, w_value, w_out):
    seq_count = tokens.shape[0]
    seq_len = tokens.shape[1]
    head_dim = w_query.shape[2]
    normed = rms_norm(tokens).astype(jnp.bfloat16)
    query = jnp.einsum('bsd,dhk->bshk', normed, w_query, preferred_element_type=jnp.float32).astype(jnp.bfloat16)
    keys = jnp.einsum('bsd,dhk->bshk', normed, w_key, preferred_element_type=jnp.float32).astype(jnp.bfloat16)
    values = jnp.einsum('bsd,dhk->bshk', normed, w_value, preferred_element_type=jnp.float32).astype(jnp.bfloat16)
    scores = jnp.einsum('bqhk,bshk->bhqs', query, keys, preferred_element_type=jnp.float32) * head_dim ** -0.5
    causal = lax.broadcasted_iota(jnp.int32, (seq_len, seq_len), 0) >= lax.broadcasted_iota(jnp.int32, (seq_len, seq_len), 1)
    attn_weights = jax.nn.softmax(jnp.where(causal, scores, -jnp.inf), axis=-1).astype(jnp.bfloat16)
    context = jnp.einsum('bhqs,bshk->bqhk', attn_weights, values, preferred_element_type=jnp.float32).astype(jnp.bfloat16)
    attn_out = jnp.einsum('crd,de->cre', context.reshape(seq_count, seq_len, -1), w_out, preferred_element_type=jnp.float32)
    return (tokens.astype(jnp.float32) + attn_out).astype(jnp.bfloat16)


def router_gates(hidden, w_router, expert_ids):
    normed = rms_norm(hidden)
    logits = jnp.dot(normed, w_router, precision=lax.Precision.HIGHEST, preferred_element_type=jnp.float32)
    picks = []
    lane = lax.broadcasted_iota(jnp.int32, logits.shape, 1)
    for j in range(expert_ids.shape[1]):
        picks.append(jnp.sum(jnp.where(lane == expert_ids[:, j:j + 1], logits, 0.0), axis=1))
    chosen = jnp.stack(picks, axis=1)
    return normed.astype(jnp.bfloat16), jax.nn.softmax(chosen, axis=-1)


def routing_tables(ids_all, base, local_experts, group):
    total, choices = ids_all.shape
    per_dev = total // group
    loc = (ids_all - base).reshape(group, per_dev, choices)
    eq = loc[:, :, :, None] == jnp.arange(local_experts, dtype=jnp.int32)
    tok = lax.broadcasted_iota(jnp.int32, (group, per_dev, choices), 0) * per_dev + lax.broadcasted_iota(jnp.int32, (group, per_dev, choices), 1)
    pack = lax.broadcasted_iota(jnp.int32, (group, per_dev, choices), 2) * (2 * total) + tok
    code = jnp.sum(jnp.where(eq, pack[:, :, :, None], 0), axis=2)
    member = jnp.sum(eq.astype(jnp.int32), axis=2)
    tri = (lax.broadcasted_iota(jnp.int32, (per_dev, per_dev), 0) > lax.broadcasted_iota(jnp.int32, (per_dev, per_dev), 1)).astype(jnp.bfloat16)
    before = jnp.einsum('uv,sve->sue', tri, member.astype(jnp.bfloat16), preferred_element_type=jnp.float32).astype(jnp.int32)
    place = jnp.where(member > 0, before, -1)
    slot = jnp.arange(CAP, dtype=jnp.int32)
    short = jnp.sum(jnp.where(place[:, :, None, :] == slot[None, None, :, None], code[:, :, None, :], 0), axis=1)
    counts = jnp.sum(member, axis=1)
    offs = jnp.cumsum(counts, axis=0) - counts
    dest = jnp.where(slot[None, :, None] < counts[:, None, :], offs[:, None, :] + slot[None, :, None], -1)
    cap_all = group * CAP
    dest = dest.reshape(group * CAP, local_experts)
    short = short.reshape(group * CAP, local_experts)
    hit = dest[:, :, None] == jnp.arange(cap_all, dtype=jnp.int32)
    table = jnp.sum(jnp.where(hit, short[:, :, None] + 1, 0), axis=0) - 1
    table = jnp.where(table < 0, total, table)
    return table, jnp.sum(counts, axis=0)


def moe_kernel(sizes, codes, counts, gates, u_hbm, w1_ref, w3_ref, w2_ref, out_hbm, u_ref, acc, xrow, xmat, orow, sem):
    total, cap_all, sub = sizes
    e = pl.program_id(0)
    mask = 2 * total - 1
    shift = (2 * total).bit_length() - 1

    @pl.when(e == 0)
    def _():
        load = pltpu.make_async_copy(u_hbm, u_ref.at[pl.ds(0, total)], sem)
        load.start()
        u_ref[pl.ds(total, 1)] = jnp.zeros((1,) + u_ref.shape[1:], u_ref.dtype)

        def clear(i, _):
            acc[pl.ds(i * 8, 8)] = jnp.zeros((8,) + acc.shape[1:], acc.dtype)
            return 0

        lax.fori_loop(0, total // 8, clear, 0)
        load.wait()

    rows = counts[e]
    blocks = (rows + (BATCH - 1)) // BATCH

    def gather(b, _):
        first = pl.multiple_of(b * BATCH, BATCH)
        for k in range(BATCH):
            t = codes[e * cap_all + first + k] & mask
            xrow[pl.ds(pl.multiple_of((first + k) * sub, sub), sub), :] = u_ref[t].astype(jnp.float32)
        return 0

    lax.fori_loop(0, blocks, gather, 0)

    def ffn(m):
        for c in range(sub):
            xmat[pl.ds(0, m), c * LANES:(c + 1) * LANES] = xrow[pl.ds(c, m, stride=sub), :].astype(jnp.bfloat16)
        w13 = jnp.concatenate([w1_ref[0], w3_ref[0]], axis=1)
        both = jnp.dot(xmat[pl.ds(0, m), :], w13, preferred_element_type=jnp.float32)
        first, third = both[:, :LANES], both[:, LANES:]
        act = (first * jax.nn.sigmoid(first) * third).astype(jnp.bfloat16)
        done = jnp.dot(act, w2_ref[0], preferred_element_type=jnp.float32)
        for c in range(sub):
            part = done[:, c * LANES:(c + 1) * LANES].astype(jnp.bfloat16).astype(jnp.float32)
            orow[pl.ds(c, m, stride=sub), :] = part

    steps = (48, 96, cap_all)
    low = 0
    for m in steps:
        @pl.when((rows > low) & (rows <= m))
        def _(m=m):
            ffn(m)
        low = m

    def scatter(b, _):
        first = pl.multiple_of(b * BATCH, BATCH)
        toks, vals = [], []
        for k in range(BATCH):
            code = codes[e * cap_all + first + k]
            t = code & mask
            g = gates[(code >> shift) * total + t]
            toks.append(t)
            vals.append(acc[t] + g * orow[pl.ds(pl.multiple_of((first + k) * sub, sub), sub), :])
        for k in range(BATCH):
            acc[toks[k]] = vals[k]
        return 0

    lax.fori_loop(0, blocks, scatter, 0)

    @pl.when(e == pl.num_programs(0) - 1)
    def _():
        store = pltpu.make_async_copy(acc.at[pl.ds(0, total)], out_hbm, sem)
        store.start()
        store.wait()


def moe_partial(u_rows, gates_flat, codes, counts, w_one, w_three, w_two):
    total, sub, _ = u_rows.shape
    local, model_dim, ff = w_one.shape
    cap_all = codes.shape[0] // local
    return pl.pallas_call(
        functools.partial(moe_kernel, (total, cap_all, sub)),
        out_shape=jax.ShapeDtypeStruct((total, sub, LANES), jnp.float32),
        grid=(local,),
        in_specs=[
            pl.BlockSpec(memory_space=pltpu.SMEM),
            pl.BlockSpec(memory_space=pltpu.SMEM),
            pl.BlockSpec(memory_space=pltpu.SMEM),
            pl.BlockSpec(memory_space=pl.ANY),
            pl.BlockSpec((1, model_dim, ff), lambda e: (e, 0, 0)),
            pl.BlockSpec((1, model_dim, ff), lambda e: (e, 0, 0)),
            pl.BlockSpec((1, ff, model_dim), lambda e: (e, 0, 0)),
        ],
        out_specs=pl.BlockSpec(memory_space=pl.ANY),
        scratch_shapes=[
            pltpu.VMEM((total + 8, sub, LANES), jnp.bfloat16),
            pltpu.VMEM((total + 8, sub, LANES), jnp.float32),
            pltpu.VMEM((cap_all * sub, LANES), jnp.float32),
            pltpu.VMEM((cap_all, model_dim), jnp.bfloat16),
            pltpu.VMEM((cap_all * sub, LANES), jnp.float32),
            pltpu.SemaphoreType.DMA,
        ],
        compiler_params=pltpu.CompilerParams(dimension_semantics=('arbitrary',), vmem_limit_bytes=67043328),
        cost_estimate=pl.CostEstimate(flops=6 * 96 * local * model_dim * ff, bytes_accessed=150_000_000, transcendentals=0),
        name='moe_partial',
    )(codes, counts, gates_flat, u_rows, w_one, w_three, w_two)


def solution(mesh):
    tok_spec = P(('dp', 'ep'))
    row_spec = P('ep')
    group = mesh.shape['ep']

    def local_layer(tokens, w_query, w_key, w_value, w_out, w_router, w_one, w_three, w_two, expert_ids):
        seq_count, seq_len, model_dim = tokens.shape
        choices = expert_ids.shape[2]
        tok_count = seq_count * seq_len
        local = w_one.shape[0]
        ids = expert_ids.reshape(tok_count, choices)
        ids_all = lax.all_gather(ids, 'ep', axis=0, tiled=True)
        codes, counts = routing_tables(ids_all, lax.axis_index('ep') * local, local, group)
        full_query = lax.all_gather(w_query, 'ep', axis=0, tiled=True)
        full_key = lax.all_gather(w_key, 'ep', axis=0, tiled=True)
        full_value = lax.all_gather(w_value, 'ep', axis=0, tiled=True)
        full_out = lax.all_gather(w_out, 'ep', axis=0, tiled=True)
        hidden = attention_layer(tokens, full_query, full_key, full_value, full_out).reshape(tok_count, model_dim)
        normed, gates = router_gates(hidden, w_router, ids)
        u_rows = lax.all_gather(normed.reshape(tok_count, model_dim // LANES, LANES), 'ep', axis=0, tiled=True)
        gates_all = lax.all_gather(gates.T, 'ep', axis=1, tiled=True)
        partial = moe_partial(u_rows, gates_all.reshape(-1), codes.reshape(-1), counts, w_one, w_three, w_two)
        mixed = lax.psum_scatter(partial, 'ep', scatter_dimension=0, tiled=True)
        layer_out = (hidden.astype(jnp.float32) + mixed.reshape(tok_count, model_dim)).astype(jnp.bfloat16)
        return layer_out.reshape(seq_count, seq_len, model_dim)

    return jax.shard_map(local_layer, mesh=mesh, in_specs=(tok_spec, row_spec, row_spec, row_spec, row_spec, P(), row_spec, row_spec, row_spec, tok_spec), out_specs=tok_spec, check_vma=False)
```

```python
import functools

import jax
import jax.numpy as jnp
from jax import lax
from jax.experimental import pallas as pl
from jax.experimental.pallas import tpu as pltpu
from jax.sharding import PartitionSpec as P

EPS = 1e-6
CAP = 20
LANES = 128
BATCH = 8
CORE, ALONG_X, ALONG_Y = 1, 2, 4


def rms_norm(vals):
    wide = vals.astype(jnp.float32)
    return wide * lax.rsqrt(jnp.mean(wide * wide, axis=-1, keepdims=True) + EPS)


def hop(vals, bit):
    return lax.ppermute(vals, 'ep', [(i, i ^ bit) for i in range(8)])


def tie(vals, *others):
    return lax.optimization_barrier((vals,) + others)[0] if others else vals


class Spread:
    def __init__(self, block, *after):
        self.half = block.shape[0] // 2
        self.block = tie(block, *after)
        self.upper, self.lower = self.block[:self.half], self.block[self.half:]
        self.upper2 = hop(self.upper, ALONG_X)
        self.lower4 = hop(self.lower, ALONG_Y)
        self.lower2 = hop(self.lower, ALONG_X)
        self.upper4 = hop(self.upper, ALONG_Y)

    def forward(self, *after):
        self.upper6 = hop(tie(self.upper2, *after), ALONG_Y)
        self.lower6 = hop(tie(self.lower4, *after), ALONG_X)

    def pieces(self, *after):
        half = self.half
        found = [(0, 0, self.block), (1, 0, hop(tie(self.block, *after), CORE))]
        for bits, start, part in ((2, 0, self.upper2), (4, half, self.lower4), (2, half, self.lower2), (4, 0, self.upper4), (6, 0, self.upper6), (6, half, self.lower6)):
            found.append((bits, start, part))
            found.append((bits ^ CORE, start, hop(tie(part, *after), CORE)))
        return found


def spread_small(block, axis):
    return jnp.concatenate([block] + [hop(block, bits) for bits in range(1, 8)], axis=axis)


def matmul_kernel(count, rows_ref, *refs):
    weight = jnp.concatenate([ref[...] for ref in refs[:count]], axis=0)
    total = jnp.dot(rows_ref[...], weight, preferred_element_type=jnp.float32)
    if len(refs) == count + 2:
        total = refs[count][...].astype(jnp.float32) + total
    refs[-1][...] = total.astype(jnp.bfloat16)


def piece_matmul(rows, pieces, residual, name):
    m, depth = rows.shape
    cols = pieces[0].shape[1]
    tile = 512
    extra = [] if residual is None else [residual]
    specs = [pl.BlockSpec((m, depth), lambda j: (0, 0))]
    specs += [pl.BlockSpec((p.shape[0], tile), lambda j: (0, j)) for p in pieces]
    specs += [pl.BlockSpec((m, tile), lambda j: (0, j)) for _ in extra]
    return pl.pallas_call(
        functools.partial(matmul_kernel, len(pieces)),
        out_shape=jax.ShapeDtypeStruct((m, cols), jnp.bfloat16),
        grid=(cols // tile,),
        in_specs=specs,
        out_specs=pl.BlockSpec((m, tile), lambda j: (0, j)),
        compiler_params=pltpu.CompilerParams(dimension_semantics=('arbitrary',), vmem_limit_bytes=40 * 1024 * 1024),
        cost_estimate=pl.CostEstimate(flops=2 * m * depth * cols, bytes_accessed=2 * depth * cols, transcendentals=0),
        name=name,
    )(rows, *pieces, *extra)


def flash_kernel(scale, order_ref, q_ref, k_ref, v_ref, out_ref):
    length = q_ref.shape[0]
    scores = lax.dot_general(q_ref[...], k_ref[...], (((1,), (1,)), ((), ())), preferred_element_type=jnp.float32) * scale
    seen = lax.broadcasted_iota(jnp.int32, (length, length), 0) >= lax.broadcasted_iota(jnp.int32, (length, length), 1)
    scores = jnp.where(seen, scores, -jnp.inf)
    grown = jnp.exp(scores - jnp.max(scores, axis=1, keepdims=True))
    probs = (grown / jnp.sum(grown, axis=1, keepdims=True)).astype(jnp.bfloat16)
    out_ref[...] = jnp.dot(probs, v_ref[...], preferred_element_type=jnp.float32).astype(jnp.bfloat16)


def flash(query, keys, values, order, head_dim):
    length, width = query.shape
    heads = width // head_dim
    pick = pl.BlockSpec((length, head_dim), lambda h, order: (0, order[h]))
    return pl.pallas_call(
        functools.partial(flash_kernel, head_dim ** -0.5),
        out_shape=jax.ShapeDtypeStruct((length, width), jnp.bfloat16),
        grid_spec=pltpu.PrefetchScalarGridSpec(
            num_scalar_prefetch=1,
            grid=(heads,),
            in_specs=[pick, pick, pick],
            out_specs=pl.BlockSpec((length, head_dim), lambda h, order: (0, h)),
        ),
        compiler_params=pltpu.CompilerParams(dimension_semantics=('arbitrary',), vmem_limit_bytes=40 * 1024 * 1024),
        cost_estimate=pl.CostEstimate(flops=4 * length * length * width, bytes_accessed=8 * length * width, transcendentals=heads * length * length),
        name='flash',
    )(order, query, keys, values)


def router_gates(hidden, w_router, expert_ids):
    normed = rms_norm(hidden)
    logits = jnp.dot(normed, w_router, precision=lax.Precision.HIGHEST, preferred_element_type=jnp.float32)
    picks = []
    lane = lax.broadcasted_iota(jnp.int32, logits.shape, 1)
    for j in range(expert_ids.shape[1]):
        picks.append(jnp.sum(jnp.where(lane == expert_ids[:, j:j + 1], logits, 0.0), axis=1))
    chosen = jnp.stack(picks, axis=1)
    return normed.astype(jnp.bfloat16), jax.nn.softmax(chosen, axis=-1)


def routing_tables(ids_all, base, local_experts, group):
    total, choices = ids_all.shape
    per_dev = total // group
    loc = (ids_all - base).reshape(group, per_dev, choices)
    eq = loc[:, :, :, None] == jnp.arange(local_experts, dtype=jnp.int32)
    tok = lax.broadcasted_iota(jnp.int32, (group, per_dev, choices), 0) * per_dev + lax.broadcasted_iota(jnp.int32, (group, per_dev, choices), 1)
    pack = lax.broadcasted_iota(jnp.int32, (group, per_dev, choices), 2) * (2 * total) + tok
    code = jnp.sum(jnp.where(eq, pack[:, :, :, None], 0), axis=2)
    member = jnp.sum(eq.astype(jnp.int32), axis=2)
    tri = (lax.broadcasted_iota(jnp.int32, (per_dev, per_dev), 0) > lax.broadcasted_iota(jnp.int32, (per_dev, per_dev), 1)).astype(jnp.bfloat16)
    before = jnp.einsum('uv,sve->sue', tri, member.astype(jnp.bfloat16), preferred_element_type=jnp.float32).astype(jnp.int32)
    place = jnp.where(member > 0, before, -1)
    slot = jnp.arange(CAP, dtype=jnp.int32)
    short = jnp.sum(jnp.where(place[:, :, None, :] == slot[None, None, :, None], code[:, :, None, :], 0), axis=1)
    counts = jnp.sum(member, axis=1)
    offs = jnp.cumsum(counts, axis=0) - counts
    dest = jnp.where(slot[None, :, None] < counts[:, None, :], offs[:, None, :] + slot[None, :, None], -1)
    cap_all = group * CAP
    dest = dest.reshape(group * CAP, local_experts)
    short = short.reshape(group * CAP, local_experts)
    hit = dest[:, :, None] == jnp.arange(cap_all, dtype=jnp.int32)
    table = jnp.sum(jnp.where(hit, short[:, :, None] + 1, 0), axis=0) - 1
    table = jnp.where(table < 0, total, table)
    return table, jnp.sum(counts, axis=0)


def by_size(rows, cap_all, work):
    low = 0
    for m in (48, 96, cap_all):
        @pl.when((rows > low) & (rows <= m))
        def _(m=m):
            work(m)
        low = m


def moe_kernel(sizes, places, codes, counts, gates, *refs):
    total, cap_all, sub, per_dev = sizes
    count = len(places)
    pieces = refs[:count]
    w1_ref, w3_ref, w2_ref, keep_hbm, send_hbm, u_ref, acc, xrow, xmat, orow, sems = refs[count:]
    e = pl.program_id(0)
    mask = 2 * total - 1
    shift = (2 * total).bit_length() - 1

    @pl.when(e == 0)
    def _():
        loads = [pltpu.make_async_copy(piece, u_ref.at[pl.ds(place, piece.shape[0])], sems.at[i]) for i, (place, piece) in enumerate(zip(places, pieces))]
        for copy in loads:
            copy.start()
        u_ref[pl.ds(total, 1)] = jnp.zeros((1,) + u_ref.shape[1:], u_ref.dtype)

        def clear(i, _):
            acc[pl.ds(i * 8, 8)] = jnp.zeros((8,) + acc.shape[1:], acc.dtype)
            return 0

        lax.fori_loop(0, total // 8, clear, 0)
        for copy in loads:
            copy.wait()

    rows = counts[e]
    blocks = (rows + (BATCH - 1)) // BATCH

    def gather(b, _):
        first = pl.multiple_of(b * BATCH, BATCH)
        for k in range(BATCH):
            t = codes[e * cap_all + first + k] & mask
            xrow[pl.ds(pl.multiple_of((first + k) * sub, sub), sub), :] = u_ref[t].astype(jnp.float32)
        return 0

    lax.fori_loop(0, blocks, gather, 0)

    def ffn(m):
        for c in range(sub):
            xmat[pl.ds(0, m), c * LANES:(c + 1) * LANES] = xrow[pl.ds(c, m, stride=sub), :].astype(jnp.bfloat16)
        w13 = jnp.concatenate([w1_ref[0], w3_ref[0]], axis=1)
        both = jnp.dot(xmat[pl.ds(0, m), :], w13, preferred_element_type=jnp.float32)
        first, third = both[:, :LANES], both[:, LANES:]
        act = (first * jax.nn.sigmoid(first) * third).astype(jnp.bfloat16)
        done = jnp.dot(act, w2_ref[0], preferred_element_type=jnp.float32)
        for c in range(sub):
            orow[pl.ds(c, m, stride=sub), :] = done[:, c * LANES:(c + 1) * LANES].astype(jnp.bfloat16).astype(jnp.float32)

    by_size(rows, cap_all, ffn)

    def scatter(b, _):
        first = pl.multiple_of(b * BATCH, BATCH)
        toks, vals = [], []
        for k in range(BATCH):
            code = codes[e * cap_all + first + k]
            t = code & mask
            g = gates[(code >> shift) * total + t]
            toks.append(t)
            vals.append(acc[t] + g * orow[pl.ds(pl.multiple_of((first + k) * sub, sub), sub), :])
        for k in range(BATCH):
            acc[toks[k]] = vals[k]
        return 0

    lax.fori_loop(0, blocks, scatter, 0)

    @pl.when(e == pl.num_programs(0) - 1)
    def _():
        stores = []
        for k in range(total // per_dev):
            out = send_hbm if k % 2 else keep_hbm
            stores.append(pltpu.make_async_copy(acc.at[pl.ds(k * per_dev, per_dev)], out.at[k // 2], sems.at[k]))
        for copy in stores:
            copy.start()
        for copy in stores:
            copy.wait()


def moe_partial(per_dev, codes, counts, gates_flat, places, pieces, w_one, w_three, w_two):
    local, ff, model_dim = w_two.shape
    cap_all = codes.shape[0] // local
    sub = model_dim // LANES
    total = per_dev * 8
    smem = pl.BlockSpec(memory_space=pltpu.SMEM)
    hbm = pl.BlockSpec(memory_space=pl.ANY)
    in_spec = pl.BlockSpec((1, model_dim, ff), lambda e: (e, 0, 0))
    sums = jax.ShapeDtypeStruct((4, per_dev, sub, LANES), jnp.float32)
    return pl.pallas_call(
        functools.partial(moe_kernel, (total, cap_all, sub, per_dev), places),
        out_shape=(sums, sums),
        grid=(local,),
        in_specs=[smem] * 3 + [hbm] * len(pieces) + [in_spec, in_spec, pl.BlockSpec((1, ff, model_dim), lambda e: (e, 0, 0))],
        out_specs=(hbm, hbm),
        scratch_shapes=[
            pltpu.VMEM((total + 8, sub, LANES), jnp.bfloat16),
            pltpu.VMEM((total + 8, sub, LANES), jnp.float32),
            pltpu.VMEM((cap_all * sub, LANES), jnp.float32),
            pltpu.VMEM((cap_all, model_dim), jnp.bfloat16),
            pltpu.VMEM((cap_all * sub, LANES), jnp.float32),
            pltpu.SemaphoreType.DMA((16,)),
        ],
        compiler_params=pltpu.CompilerParams(dimension_semantics=('arbitrary',), vmem_limit_bytes=67043328),
        cost_estimate=pl.CostEstimate(flops=60_000_000_000, bytes_accessed=150_000_000, transcendentals=0),
        name='moe_partial',
    )(codes, counts, gates_flat, *pieces, w_one, w_three, w_two)


def collect_kernel(parts, keep_hbm, send_hbm, resid_ref, out_ref, near, sums, chip_in, last_in, load_sems, sems_a, sems_b, sems_c):
    me = lax.axis_index('ep')
    core = me + 1 - 2 * (me % 2)
    along_x = me + 2 - 4 * ((me // 2) % 2)
    along_y = me + 4 - 8 * (me // 4)
    height = sums.shape[1] // parts
    sub = sums.shape[1] // out_ref.shape[0]

    barrier = pltpu.get_barrier_semaphore()
    for other in (core, along_x, along_y):
        pl.semaphore_signal(barrier, inc=1, device_id={'ep': other}, device_id_type=pl.DeviceIdType.MESH)
    pl.semaphore_wait(barrier, 3)

    def part(i):
        return pl.ds(pl.multiple_of(i * height, height), height)

    def load(i):
        return pltpu.make_async_copy(keep_hbm.at[:, part(i)], sums.at[:, part(i)], load_sems.at[i])

    def remote(src, dst, sems, slot, other):
        return pltpu.make_async_remote_copy(src_ref=src, dst_ref=dst, send_sem=sems.at[0, slot], recv_sem=sems.at[1, slot], device_id={'ep': other}, device_id_type=pl.DeviceIdType.MESH)

    def to_core(i):
        return remote(send_hbm.at[:, part(i)], near.at[:, part(i)], sems_a, i, core)

    def to_chip(i, kind):
        sent = (1, 3) if kind == 0 else (2, 3)
        other = along_x if kind == 0 else along_y
        return [remote(sums.at[k, part(i)], chip_in.at[n, part(i)], sems_b, i * 2 + n, other) for n, k in enumerate(sent)]

    def to_last(i, kind):
        k, other = (2, along_y) if kind == 0 else (1, along_x)
        return remote(sums.at[k, part(i)], last_in.at[part(i)], sems_c, i, other)

    def start(i, _):
        to_core(i).start()
        load(i).start()
        return 0

    lax.fori_loop(0, parts, start, 0)

    def first(pair, _):
        for kind in range(2):
            i = pair * 2 + kind
            load(i).wait()
            to_core(i).wait_recv()
            for k in (1, 3, 2, 0):
                sums[k, part(i)] += near[k, part(i)]
            for copy in to_chip(i, kind):
                copy.start()
        return 0

    lax.fori_loop(0, parts // 2, first, 0)

    def second(pair, _):
        for kind in range(2):
            i = pair * 2 + kind
            for copy in to_chip(i, kind):
                copy.wait_recv()
            k = 2 if kind == 0 else 1
            sums[k, part(i)] += chip_in[1, part(i)]
            to_last(i, kind).start()
            sums[0, part(i)] += chip_in[0, part(i)]
        return 0

    lax.fori_loop(0, parts // 2, second, 0)

    def third(pair, _):
        for kind in range(2):
            i = pair * 2 + kind
            to_last(i, kind).wait_recv()
            sums[0, part(i)] += last_in[part(i)]
            tokens = height // sub
            rows = pl.ds(pl.multiple_of(i * tokens, tokens), tokens)
            for c in range(sub):
                cols = slice(c * LANES, (c + 1) * LANES)
                mixed = sums[0, pl.ds(i * height + c, tokens, stride=sub), :]
                out_ref[rows, cols] = (resid_ref[rows, cols].astype(jnp.float32) + mixed).astype(jnp.bfloat16)
            to_core(i).wait_send()
            for copy in to_chip(i, kind):
                copy.wait_send()
            to_last(i, kind).wait_send()
        return 0

    lax.fori_loop(0, parts // 2, third, 0)


def collect(keep, send, resid, parts=16):
    tokens, model_dim = resid.shape
    rows = keep.shape[1] * keep.shape[2]
    keep = keep.reshape(4, rows, LANES)
    send = send.reshape(4, rows, LANES)
    hbm = pl.BlockSpec(memory_space=pl.ANY)
    vmem = pl.BlockSpec(memory_space=pltpu.VMEM)
    return pl.pallas_call(
        functools.partial(collect_kernel, parts),
        out_shape=jax.ShapeDtypeStruct((tokens, model_dim), jnp.bfloat16),
        in_specs=[hbm, hbm, vmem],
        out_specs=vmem,
        scratch_shapes=[
            pltpu.VMEM((4, rows, LANES), jnp.float32),
            pltpu.VMEM((4, rows, LANES), jnp.float32),
            pltpu.VMEM((2, rows, LANES), jnp.float32),
            pltpu.VMEM((rows, LANES), jnp.float32),
            pltpu.SemaphoreType.DMA((parts,)),
            pltpu.SemaphoreType.DMA((2, parts)),
            pltpu.SemaphoreType.DMA((2, parts * 2)),
            pltpu.SemaphoreType.DMA((2, parts)),
        ],
        compiler_params=pltpu.CompilerParams(collective_id=0, has_side_effects=True, vmem_limit_bytes=60 * 1024 * 1024),
        cost_estimate=pl.CostEstimate(flops=100_000_000, bytes_accessed=40_000_000, transcendentals=0),
        name='collect',
    )(keep, send, resid)


def solution(mesh):
    tok_spec = P(('dp', 'ep'))
    row_spec = P('ep')
    group = mesh.shape['ep']

    def local_layer(tokens, w_query, w_key, w_value, w_out, w_router, w_one, w_three, w_two, expert_ids):
        seq_count, seq_len, model_dim = tokens.shape
        choices = expert_ids.shape[2]
        tok_count = seq_count * seq_len
        local = w_one.shape[0]
        head_dim = w_query.shape[2]
        me = lax.axis_index('ep')
        ids = expert_ids.reshape(tok_count, choices)
        flat = tokens.reshape(tok_count, model_dim)
        normed = rms_norm(flat).astype(jnp.bfloat16)
        rows = w_query.shape[0]
        ids_all = spread_small(ids, 0)
        codes, counts = routing_tables(ids_all, me * local, local, group)
        query_in = Spread(w_query.reshape(rows, -1), ids_all)
        query_in.forward()
        key_in = Spread(w_key.reshape(rows, -1), query_in.upper2, query_in.lower4)
        key_in.forward()
        value_in = Spread(w_value.reshape(rows, -1), key_in.upper2, key_in.lower4)
        parts = query_in.pieces()
        mixed_rows = jnp.concatenate([lax.dynamic_slice_in_dim(normed, (me ^ bits) * rows + start, part.shape[0], axis=1) for bits, start, part in parts], axis=1)
        query = piece_matmul(mixed_rows, [part for _, _, part in parts], None, 'query')
        value_in.forward(query)
        keys = piece_matmul(mixed_rows, [part for _, _, part in key_in.pieces()], None, 'key')
        out_in = Spread(w_out, query)
        out_in.forward(keys)
        values = piece_matmul(mixed_rows, [part for _, _, part in value_in.pieces()], None, 'value')
        order = []
        for bits, start, part in parts:
            scaled = start * w_out.shape[0] // rows
            for step in range(part.shape[0] * w_out.shape[0] // rows // head_dim):
                order.append((me ^ bits) * (w_out.shape[0] // head_dim) + scaled // head_dim + step)
        context = flash(query, keys, values, jnp.stack(order).astype(jnp.int32), head_dim)
        out_parts = out_in.pieces(context)
        hidden = piece_matmul(context, [part for _, _, part in out_parts], flat, 'out')

        normed_h, gates = router_gates(hidden, w_router, ids)
        u_in = Spread(normed_h.reshape(tok_count, model_dim // LANES, LANES))
        u_in.forward()
        u_parts = u_in.pieces()
        gates_flat = spread_small(gates.T, 1).reshape(-1)
        codes = codes.reshape(-1)
        places = [bits * tok_count + start for bits, start, _ in u_parts]
        keep, send = moe_partial(tok_count, codes, counts, gates_flat, places, [part for _, _, part in u_parts], w_one, w_three, w_two)
        layer_out = collect(keep, send, hidden)
        return layer_out.reshape(seq_count, seq_len, model_dim)

    return jax.shard_map(local_layer, mesh=mesh, in_specs=(tok_spec, row_spec, row_spec, row_spec, row_spec, P(), row_spec, row_spec, row_spec, tok_spec), out_specs=tok_spec, check_vma=False)
```

```python
import functools

import jax
import jax.numpy as jnp
from jax import lax
from jax.experimental import pallas as pl
from jax.experimental.pallas import tpu as pltpu
from jax.sharding import PartitionSpec as P

EPS = 1e-6
CAP = 20
LANES = 128
BATCH = 8
CORE, ALONG_X, ALONG_Y = 1, 2, 4


def rms_norm(vals):
    wide = vals.astype(jnp.float32)
    return wide * lax.rsqrt(jnp.mean(wide * wide, axis=-1, keepdims=True) + EPS)


def hop(vals, bit):
    return lax.ppermute(vals, 'ep', [(i, i ^ bit) for i in range(8)])


def tie(vals, *others):
    return lax.optimization_barrier((vals,) + others)[0] if others else vals


class Spread:
    def __init__(self, block, *after):
        self.half = block.shape[0] // 2
        self.block = tie(block, *after)
        self.upper, self.lower = self.block[:self.half], self.block[self.half:]
        self.upper2 = hop(self.upper, ALONG_X)
        self.lower4 = hop(self.lower, ALONG_Y)
        self.lower2 = hop(self.lower, ALONG_X)
        self.upper4 = hop(self.upper, ALONG_Y)

    def forward(self, *after):
        self.upper6 = hop(tie(self.upper2, *after), ALONG_Y)
        self.lower6 = hop(tie(self.lower4, *after), ALONG_X)

    def pieces(self, early=(), late=()):
        half = self.half
        found = [(0, 0, self.block), (1, 0, hop(tie(self.block, *early), CORE))]
        for bits, start, part in ((2, 0, self.upper2), (4, half, self.lower4), (2, half, self.lower2), (4, 0, self.upper4), (6, 0, self.upper6), (6, half, self.lower6)):
            found.append((bits, start, part))
            found.append((bits ^ CORE, start, hop(tie(part, *(late if bits == 6 else early)), CORE)))
        return found


def spread_small(block, axis):
    return jnp.concatenate([block] + [hop(block, bits) for bits in range(1, 8)], axis=axis)


def matmul_kernel(count, rows_ref, *refs):
    weight = jnp.concatenate([ref[...] for ref in refs[:count]], axis=0)
    total = jnp.dot(rows_ref[...], weight, preferred_element_type=jnp.float32)
    if len(refs) == count + 2:
        total = refs[count][...].astype(jnp.float32) + total
    refs[-1][...] = total.astype(refs[-1].dtype)


def piece_matmul(rows, pieces, residual, name, block=0, dtype=jnp.bfloat16):
    m = rows.shape[0]
    depth = sum(p.shape[0] for p in pieces)
    cols = pieces[0].shape[1]
    tile = 512
    extra = [] if residual is None else [residual]
    specs = [pl.BlockSpec((m, depth), lambda j: (0, block))]
    specs += [pl.BlockSpec((p.shape[0], tile), lambda j: (0, j)) for p in pieces]
    specs += [pl.BlockSpec((m, tile), lambda j: (0, j)) for _ in extra]
    return pl.pallas_call(
        functools.partial(matmul_kernel, len(pieces)),
        out_shape=jax.ShapeDtypeStruct((m, cols), dtype),
        grid=(cols // tile,),
        in_specs=specs,
        out_specs=pl.BlockSpec((m, tile), lambda j: (0, j)),
        compiler_params=pltpu.CompilerParams(dimension_semantics=('arbitrary',), vmem_limit_bytes=67043328),
        cost_estimate=pl.CostEstimate(flops=2 * m * depth * cols, bytes_accessed=2 * depth * cols, transcendentals=0),
        name=name,
    )(rows, *pieces, *extra)


def flash_kernel(scale, order_ref, q_ref, k_ref, v_ref, out_ref):
    length = q_ref.shape[0]
    scores = lax.dot_general(q_ref[...], k_ref[...], (((1,), (1,)), ((), ())), preferred_element_type=jnp.float32) * scale
    seen = lax.broadcasted_iota(jnp.int32, (length, length), 0) >= lax.broadcasted_iota(jnp.int32, (length, length), 1)
    scores = jnp.where(seen, scores, -jnp.inf)
    grown = jnp.exp(scores - jnp.max(scores, axis=1, keepdims=True))
    probs = (grown / jnp.sum(grown, axis=1, keepdims=True)).astype(jnp.bfloat16)
    out_ref[...] = jnp.dot(probs, v_ref[...], preferred_element_type=jnp.float32).astype(jnp.bfloat16)


def flash(query, keys, values, order, head_dim):
    length, width = query.shape
    heads = width // head_dim
    pick = pl.BlockSpec((length, head_dim), lambda h, order: (0, order[h]))
    return pl.pallas_call(
        functools.partial(flash_kernel, head_dim ** -0.5),
        out_shape=jax.ShapeDtypeStruct((length, width), jnp.bfloat16),
        grid_spec=pltpu.PrefetchScalarGridSpec(
            num_scalar_prefetch=1,
            grid=(heads,),
            in_specs=[pick, pick, pick],
            out_specs=pl.BlockSpec((length, head_dim), lambda h, order: (0, h)),
        ),
        compiler_params=pltpu.CompilerParams(dimension_semantics=('arbitrary',), vmem_limit_bytes=67043328),
        cost_estimate=pl.CostEstimate(flops=4 * length * length * width, bytes_accessed=8 * length * width, transcendentals=heads * length * length),
        name='flash',
    )(order, query, keys, values)


def router_gates(hidden, w_router, expert_ids):
    normed = rms_norm(hidden)
    logits = jnp.dot(normed, w_router, precision=lax.Precision.HIGHEST, preferred_element_type=jnp.float32)
    picks = []
    lane = lax.broadcasted_iota(jnp.int32, logits.shape, 1)
    for j in range(expert_ids.shape[1]):
        picks.append(jnp.sum(jnp.where(lane == expert_ids[:, j:j + 1], logits, 0.0), axis=1))
    chosen = jnp.stack(picks, axis=1)
    return normed.astype(jnp.bfloat16), jax.nn.softmax(chosen, axis=-1)


def routing_tables(ids_all, base, local_experts, group):
    total, choices = ids_all.shape
    per_dev = total // group
    loc = (ids_all - base).reshape(group, per_dev, choices)
    eq = loc[:, :, :, None] == jnp.arange(local_experts, dtype=jnp.int32)
    tok = lax.broadcasted_iota(jnp.int32, (group, per_dev, choices), 0) * per_dev + lax.broadcasted_iota(jnp.int32, (group, per_dev, choices), 1)
    pack = lax.broadcasted_iota(jnp.int32, (group, per_dev, choices), 2) * (2 * total) + tok
    code = jnp.sum(jnp.where(eq, pack[:, :, :, None], 0), axis=2)
    member = jnp.sum(eq.astype(jnp.int32), axis=2)
    tri = (lax.broadcasted_iota(jnp.int32, (per_dev, per_dev), 0) > lax.broadcasted_iota(jnp.int32, (per_dev, per_dev), 1)).astype(jnp.bfloat16)
    before = jnp.einsum('uv,sve->sue', tri, member.astype(jnp.bfloat16), preferred_element_type=jnp.float32).astype(jnp.int32)
    place = jnp.where(member > 0, before, -1)
    slot = jnp.arange(CAP, dtype=jnp.int32)
    short = jnp.sum(jnp.where(place[:, :, None, :] == slot[None, None, :, None], code[:, :, None, :], 0), axis=1)
    counts = jnp.sum(member, axis=1)
    offs = jnp.cumsum(counts, axis=0) - counts
    dest = jnp.where(slot[None, :, None] < counts[:, None, :], offs[:, None, :] + slot[None, :, None], -1)
    cap_all = group * CAP
    dest = dest.reshape(group * CAP, local_experts)
    short = short.reshape(group * CAP, local_experts)
    hit = dest[:, :, None] == jnp.arange(cap_all, dtype=jnp.int32)
    table = jnp.sum(jnp.where(hit, short[:, :, None] + 1, 0), axis=0) - 1
    table = jnp.where(table < 0, total, table)
    return table, jnp.sum(counts, axis=0)


def by_size(rows, cap_all, work):
    low = 0
    for m in (48, 96, cap_all):
        @pl.when((rows > low) & (rows <= m))
        def _(m=m):
            work(m)
        low = m


def moe_kernel(sizes, places, codes, counts, gates, *refs):
    total, cap_all, sub, per_dev = sizes
    count = len(places)
    pieces = refs[:count]
    w1_ref, w3_ref, w2_ref, keep_hbm, send_hbm, u_ref, acc, xrow, xmat, orow, sems = refs[count:]
    e = pl.program_id(0)
    mask = 2 * total - 1
    shift = (2 * total).bit_length() - 1

    @pl.when(e == 0)
    def _():
        loads = [pltpu.make_async_copy(piece, u_ref.at[pl.ds(place, piece.shape[0])], sems.at[i]) for i, (place, piece) in enumerate(zip(places, pieces))]
        for copy in loads:
            copy.start()
        u_ref[pl.ds(total, 1)] = jnp.zeros((1,) + u_ref.shape[1:], u_ref.dtype)

        def clear(i, _):
            acc[pl.ds(i * 8, 8)] = jnp.zeros((8,) + acc.shape[1:], acc.dtype)
            return 0

        lax.fori_loop(0, total // 8, clear, 0)
        for copy in loads:
            copy.wait()

    rows = counts[e]
    blocks = (rows + (BATCH - 1)) // BATCH

    def gather(b, _):
        first = pl.multiple_of(b * BATCH, BATCH)
        for k in range(BATCH):
            t = codes[e * cap_all + first + k] & mask
            xrow[pl.ds(pl.multiple_of((first + k) * sub, sub), sub), :] = u_ref[t].astype(jnp.float32)
        return 0

    lax.fori_loop(0, blocks, gather, 0)

    def ffn(m):
        for c in range(sub):
            xmat[pl.ds(0, m), c * LANES:(c + 1) * LANES] = xrow[pl.ds(c, m, stride=sub), :].astype(jnp.bfloat16)
        w13 = jnp.concatenate([w1_ref[0], w3_ref[0]], axis=1)
        both = jnp.dot(xmat[pl.ds(0, m), :], w13, preferred_element_type=jnp.float32)
        first, third = both[:, :LANES], both[:, LANES:]
        act = (first * jax.nn.sigmoid(first) * third).astype(jnp.bfloat16)
        done = jnp.dot(act, w2_ref[0], preferred_element_type=jnp.float32)
        for c in range(sub):
            orow[pl.ds(c, m, stride=sub), :] = done[:, c * LANES:(c + 1) * LANES].astype(jnp.bfloat16).astype(jnp.float32)

    by_size(rows, cap_all, ffn)

    def scatter(b, _):
        first = pl.multiple_of(b * BATCH, BATCH)
        toks, vals = [], []
        for k in range(BATCH):
            code = codes[e * cap_all + first + k]
            t = code & mask
            g = gates[(code >> shift) * total + t]
            toks.append(t)
            vals.append(acc[t] + g * orow[pl.ds(pl.multiple_of((first + k) * sub, sub), sub), :])
        for k in range(BATCH):
            acc[toks[k]] = vals[k]
        return 0

    lax.fori_loop(0, blocks, scatter, 0)

    @pl.when(e == pl.num_programs(0) - 1)
    def _():
        stores = []
        for k in range(total // per_dev):
            out = send_hbm if k % 2 else keep_hbm
            stores.append(pltpu.make_async_copy(acc.at[pl.ds(k * per_dev, per_dev)], out.at[k // 2], sems.at[k]))
        for copy in stores:
            copy.start()
        for copy in stores:
            copy.wait()


def moe_partial(per_dev, codes, counts, gates_flat, places, pieces, w_one, w_three, w_two):
    local, ff, model_dim = w_two.shape
    cap_all = codes.shape[0] // local
    sub = model_dim // LANES
    total = per_dev * 8
    smem = pl.BlockSpec(memory_space=pltpu.SMEM)
    hbm = pl.BlockSpec(memory_space=pl.ANY)
    in_spec = pl.BlockSpec((1, model_dim, ff), lambda e: (e, 0, 0))
    sums = jax.ShapeDtypeStruct((4, per_dev, sub, LANES), jnp.float32)
    return pl.pallas_call(
        functools.partial(moe_kernel, (total, cap_all, sub, per_dev), places),
        out_shape=(sums, sums),
        grid=(local,),
        in_specs=[smem] * 3 + [hbm] * len(pieces) + [in_spec, in_spec, pl.BlockSpec((1, ff, model_dim), lambda e: (e, 0, 0))],
        out_specs=(hbm, hbm),
        scratch_shapes=[
            pltpu.VMEM((total + 8, sub, LANES), jnp.bfloat16),
            pltpu.VMEM((total + 8, sub, LANES), jnp.float32),
            pltpu.VMEM((cap_all * sub, LANES), jnp.float32),
            pltpu.VMEM((cap_all, model_dim), jnp.bfloat16),
            pltpu.VMEM((cap_all * sub, LANES), jnp.float32),
            pltpu.SemaphoreType.DMA((16,)),
        ],
        compiler_params=pltpu.CompilerParams(dimension_semantics=('arbitrary',), vmem_limit_bytes=67043328),
        cost_estimate=pl.CostEstimate(flops=60_000_000_000, bytes_accessed=150_000_000, transcendentals=0),
        name='moe_partial',
    )(codes, counts, gates_flat, *pieces, w_one, w_three, w_two)


def collect_kernel(parts, keep_hbm, send_hbm, resid_ref, out_ref, near, sums, chip_in, last_in, load_sems, sems_a, sems_b, sems_c):
    me = lax.axis_index('ep')
    core = me + 1 - 2 * (me % 2)
    along_x = me + 2 - 4 * ((me // 2) % 2)
    along_y = me + 4 - 8 * (me // 4)
    height = sums.shape[1] // parts
    sub = sums.shape[1] // out_ref.shape[0]

    barrier = pltpu.get_barrier_semaphore()
    for other in (core, along_x, along_y):
        pl.semaphore_signal(barrier, inc=1, device_id={'ep': other}, device_id_type=pl.DeviceIdType.MESH)
    pl.semaphore_wait(barrier, 3)

    def part(i):
        return pl.ds(pl.multiple_of(i * height, height), height)

    def load(i):
        return pltpu.make_async_copy(keep_hbm.at[:, part(i)], sums.at[:, part(i)], load_sems.at[i])

    def remote(src, dst, sems, slot, other):
        return pltpu.make_async_remote_copy(src_ref=src, dst_ref=dst, send_sem=sems.at[0, slot], recv_sem=sems.at[1, slot], device_id={'ep': other}, device_id_type=pl.DeviceIdType.MESH)

    def to_core(i):
        return remote(send_hbm.at[:, part(i)], near.at[:, part(i)], sems_a, i, core)

    def to_chip(i, kind):
        sent = (1, 3) if kind == 0 else (2, 3)
        other = along_x if kind == 0 else along_y
        return [remote(sums.at[k, part(i)], chip_in.at[n, part(i)], sems_b, i * 2 + n, other) for n, k in enumerate(sent)]

    def to_last(i, kind):
        k, other = (2, along_y) if kind == 0 else (1, along_x)
        return remote(sums.at[k, part(i)], last_in.at[part(i)], sems_c, i, other)

    def start(i, _):
        to_core(i).start()
        load(i).start()
        return 0

    lax.fori_loop(0, parts, start, 0)

    def first(pair, _):
        for kind in range(2):
            i = pair * 2 + kind
            load(i).wait()
            to_core(i).wait_recv()
            for k in (1, 3, 2, 0):
                sums[k, part(i)] += near[k, part(i)]
            for copy in to_chip(i, kind):
                copy.start()
        return 0

    lax.fori_loop(0, parts // 2, first, 0)

    def second(pair, _):
        for kind in range(2):
            i = pair * 2 + kind
            for copy in to_chip(i, kind):
                copy.wait_recv()
            k = 2 if kind == 0 else 1
            sums[k, part(i)] += chip_in[1, part(i)]
            to_last(i, kind).start()
            sums[0, part(i)] += chip_in[0, part(i)]
        return 0

    lax.fori_loop(0, parts // 2, second, 0)

    def third(pair, _):
        for kind in range(2):
            i = pair * 2 + kind
            to_last(i, kind).wait_recv()
            sums[0, part(i)] += last_in[part(i)]
            tokens = height // sub
            rows = pl.ds(pl.multiple_of(i * tokens, tokens), tokens)
            for c in range(sub):
                cols = slice(c * LANES, (c + 1) * LANES)
                mixed = sums[0, pl.ds(i * height + c, tokens, stride=sub), :]
                out_ref[rows, cols] = (resid_ref[rows, cols].astype(jnp.float32) + mixed).astype(jnp.bfloat16)
            to_core(i).wait_send()
            for copy in to_chip(i, kind):
                copy.wait_send()
            to_last(i, kind).wait_send()
        return 0

    lax.fori_loop(0, parts // 2, third, 0)


def collect(keep, send, resid, parts=16):
    tokens, model_dim = resid.shape
    rows = keep.shape[1] * keep.shape[2]
    keep = keep.reshape(4, rows, LANES)
    send = send.reshape(4, rows, LANES)
    hbm = pl.BlockSpec(memory_space=pl.ANY)
    vmem = pl.BlockSpec(memory_space=pltpu.VMEM)
    return pl.pallas_call(
        functools.partial(collect_kernel, parts),
        out_shape=jax.ShapeDtypeStruct((tokens, model_dim), jnp.bfloat16),
        in_specs=[hbm, hbm, vmem],
        out_specs=vmem,
        scratch_shapes=[
            pltpu.VMEM((4, rows, LANES), jnp.float32),
            pltpu.VMEM((4, rows, LANES), jnp.float32),
            pltpu.VMEM((2, rows, LANES), jnp.float32),
            pltpu.VMEM((rows, LANES), jnp.float32),
            pltpu.SemaphoreType.DMA((parts,)),
            pltpu.SemaphoreType.DMA((2, parts)),
            pltpu.SemaphoreType.DMA((2, parts * 2)),
            pltpu.SemaphoreType.DMA((2, parts)),
        ],
        compiler_params=pltpu.CompilerParams(collective_id=0, has_side_effects=True, vmem_limit_bytes=60 * 1024 * 1024),
        cost_estimate=pl.CostEstimate(flops=100_000_000, bytes_accessed=40_000_000, transcendentals=0),
        name='collect',
    )(keep, send, resid)


def solution(mesh):
    tok_spec = P(('dp', 'ep'))
    row_spec = P('ep')
    group = mesh.shape['ep']

    def local_layer(tokens, w_query, w_key, w_value, w_out, w_router, w_one, w_three, w_two, expert_ids):
        seq_count, seq_len, model_dim = tokens.shape
        choices = expert_ids.shape[2]
        tok_count = seq_count * seq_len
        local = w_one.shape[0]
        head_dim = w_query.shape[2]
        me = lax.axis_index('ep')
        ids = expert_ids.reshape(tok_count, choices)
        flat = tokens.reshape(tok_count, model_dim)
        normed = rms_norm(flat).astype(jnp.bfloat16)
        rows = w_query.shape[0]
        ids_all = spread_small(ids, 0)
        codes, counts = routing_tables(ids_all, me * local, local, group)
        query_in = Spread(w_query.reshape(rows, -1), ids_all)
        query_in.forward()
        key_in = Spread(w_key.reshape(rows, -1), query_in.upper2, query_in.lower4)
        key_in.forward()
        value_in = Spread(w_value.reshape(rows, -1), key_in.upper2, key_in.lower4)
        parts = query_in.pieces()
        mixed_rows = jnp.concatenate([lax.dynamic_slice_in_dim(normed, (me ^ bits) * rows + start, part.shape[0], axis=1) for bits, start, part in parts], axis=1)
        query = piece_matmul(mixed_rows, [part for _, _, part in parts], None, 'query')
        value_in.forward(query)
        keys = piece_matmul(mixed_rows, [part for _, _, part in key_in.pieces()], None, 'key')
        out_in = Spread(w_out, query)
        out_in.forward(keys)
        values = piece_matmul(mixed_rows, [part for _, _, part in value_in.pieces()], None, 'value')
        order = []
        for bits, start, part in parts:
            scaled = start * w_out.shape[0] // rows
            for step in range(part.shape[0] * w_out.shape[0] // rows // head_dim):
                order.append((me ^ bits) * (w_out.shape[0] // head_dim) + scaled // head_dim + step)
        context = flash(query, keys, values, jnp.stack(order).astype(jnp.int32), head_dim)
        out_parts = [part for _, _, part in out_in.pieces((values,), (context,))]
        partial = piece_matmul(context, out_parts[:-4], flat, 'out_early', 0, jnp.float32)
        hidden = piece_matmul(context, out_parts[-4:], partial, 'out_late', 3)

        normed_h, gates = router_gates(hidden, w_router, ids)
        u_in = Spread(normed_h.reshape(tok_count, model_dim // LANES, LANES))
        u_in.forward()
        gates_all = spread_small(gates.T, 1)
        u_parts = u_in.pieces((), (gates_all,))
        gates_flat = gates_all.reshape(-1)
        codes = codes.reshape(-1)
        places = [bits * tok_count + start for bits, start, _ in u_parts]
        keep, send = moe_partial(tok_count, codes, counts, gates_flat, places, [part for _, _, part in u_parts], w_one, w_three, w_two)
        layer_out = collect(keep, send, hidden)
        return layer_out.reshape(seq_count, seq_len, model_dim)

    return jax.shard_map(local_layer, mesh=mesh, in_specs=(tok_spec, row_spec, row_spec, row_spec, row_spec, P(), row_spec, row_spec, row_spec, tok_spec), out_specs=tok_spec, check_vma=False)
```
